256 devices in a mesh: section: 8 (over y, core), expert: 32 (over z, x).
Axes of the slice: x: 4, y: 4, z: 8, core: 2. Of those that a mesh axis runs over, the one named last changes fastest.
Arguments:
- tokens: bfloat16 [2, 4096, 2048], P(None, 'expert'), may hold values from -6 to 6
- norm_gain: float32 [8, 2048], P('section'), may hold values from 0.1 to 1.9
- w_gate: bfloat16 [8, 32, 2048, 704], P('section', 'expert'), may hold values from -0.125 to 0.125
- w_up: bfloat16 [8, 32, 2048, 704], P('section', 'expert'), may hold values from -0.125 to 0.125
- w_down: bfloat16 [8, 32, 704, 2048], P('section', 'expert'), may hold values from -0.21875 to 0.21875
- expert_ids: int32 [8, 2, 4096, 6], P('section', None, 'expert'), may hold values from 0 to 31, all different within a row; in each aligned block of 128 rows (0 to 127, 128 to 255, ..., all dimensions but the last counted through in order) at most 25 rows name the same one
- route_weight: float32 [8, 2, 4096, 6], P('section', None, 'expert'), may hold values from 0.1 to 1
Outputs:
- stream: bfloat16 [8, 2, 4096, 2048], P('section', None, 'expert')
The draws below stay inside these ranges and needn't reach their ends.
Inputs may be any that keep to these rules, and one draw needn't show every extreme that they name: `expert_ids`: A token names 6 different experts. In each aligned block of 128 tokens (the tokens of one device in one layer and micro-batch) no expert is named by more than 25 tokens, a bound that some block reaches.
All inputs are finite; a program needn't handle non-finite values.
Results may differ from the reference program's by a relative error of at most 0.025.
Values may be sent and summed in bfloat16 or wider, within the bound.
No kernel may reach another device: no remote copies, remote signals or barrier semaphores. Data moves between devices by JAX's collectives and lax.ppermute only.
A program may use at most 128 MiB of HBM per device.

```python
import math
import jax
import jax.numpy as jnp
import numpy as np
from jax import lax

D = 2048
HID = 704
TOP = 6
MB = 2
TOK_DEV = 128
EXPERTS = 32
LAYERS = 8
TOKENS = 4096
CAP = 25
N_EXPERT = 32


def block_scale(own_key, extent, pieces, least, high):
    loudness, own = 1.0, jax.random.fold_in(own_key, 6)
    for position, shards_of in pieces:
        draws = jnp.exp(jax.random.uniform(jax.random.fold_in(own, position), (shards_of,), jnp.float32, least / len(pieces), high / len(pieces)))
        loudness = loudness * jnp.repeat(draws, extent[position] // shards_of).reshape([-1 if axis == position else 1 for axis in range(len(extent))])
    return loudness


def deal_out(key, own, number, rows, amount, top, most, skew):
    order = jax.random.permutation(key, amount)
    heavy_load, common = load_shares(amount, rows * top, most, skew, True), load_shares(amount, rows * top, most, skew, False)
    places = jnp.arange(amount)

    def named(tallies, offset_by):
        used = int((tallies > 0).sum())
        fixed = max(1, used // 4)
        moved = fixed + (places - fixed + offset_by * (used - fixed)) % max(1, amount - fixed)
        return jnp.zeros((amount,), jnp.int32).at[order[jnp.where(places < fixed, places, moved)]].set(jnp.asarray(tallies, jnp.int32))

    tallies = jnp.where(number % 4 == 0, named(heavy_load, number // 4), named(common, number - number // 4 - 1))
    mixed = jax.random.permutation(jax.random.fold_in(own, 3), amount)
    donor, sink = mixed[0:amount // 2 * 2:2], mixed[1:amount // 2 * 2:2]
    room = jnp.minimum(tallies[donor] - 1, most - tallies[sink]) // 2
    room = jnp.where((donor == order[0]) | (sink == order[0]) | (tallies[sink] == 0), 0, jnp.maximum(room, 0))
    moved = jax.random.randint(jax.random.fold_in(own, 4), (amount // 2,), 0, 1 << 20) % (room + 1)
    tallies = tallies.at[donor].add(-moved).at[sink].add(moved)
    members = jnp.searchsorted(jnp.cumsum(tallies), jnp.arange(rows * top), side="right").astype(jnp.int32)
    listing = members.reshape(top, rows).T
    listing = listing[jax.random.permutation(jax.random.fold_in(own, 1), rows)]
    offset_by = jax.random.randint(jax.random.fold_in(own, 2), (rows, 1), 0, top)
    return jnp.take_along_axis(listing, (jnp.arange(top)[None, :] + offset_by) % top, axis=1)


def load_shares(amount, total, reach, slope, full):
    weights = [(1 << 20) // math.isqrt(grade ** slope) + 1 for grade in range(1, amount + 1)]
    largest = reach if full else min(reach, max(-(-total // amount), total * weights[0] // sum(weights)))
    least = 1 if total - largest >= amount - 1 else 0
    counts, rest = [largest] + [least] * (amount - 1), total - largest - least * (amount - 1)
    while rest > 0:
        free = [i for i in range(1, amount) if counts[i] < largest] or [i for i in range(1, amount) if counts[i] < reach]
        whole, budget = sum([weights[i] for i in free]), rest
        for i in free:
            more = min(reach - counts[i], max(1, budget * weights[i] // whole), rest)
            counts[i] = counts[i] + more
            rest = rest - more
    return np.array(counts)


def scatter_about(stream_key, shape, spread, bound, cuts=(), held_as=jnp.bfloat16):
    result = jax.random.normal(stream_key, shape, jnp.float32) * spread
    if len(cuts) > 0:
        result = block_scale(stream_key, shape, cuts, -0.22, 0.18) * result
    return jnp.clip(result, min=-bound, max=bound).astype(held_as)


def setup_inputs(seed: int = 0) -> dict:
    seeds = jax.random.split(jax.random.key(seed), 8)
    tokens = scatter_about(seeds[0], (MB, TOKENS, D), 1.0, 6.0, ((1, 32),))
    norm_gain = jnp.clip(1.0 + 0.18 * jax.random.normal(seeds[1], (LAYERS, D), jnp.float32), 0.1, 1.9)
    w_gate = scatter_about(seeds[2], (LAYERS, EXPERTS, D, HID), D ** -0.5, 0.125, ((0, 8), (1, 32)))
    w_up = scatter_about(seeds[3], (LAYERS, EXPERTS, D, HID), D ** -0.5, 0.125, ((0, 8), (1, 32)))
    w_down = scatter_about(seeds[4], (LAYERS, EXPERTS, HID, D), HID ** -0.5, 0.21875, ((0, 8), (1, 32)))
    expert_ids_keys = jax.random.split(jax.random.fold_in(seeds[5], 1), LAYERS * MB * TOKENS // TOK_DEV)
    expert_ids_turns = jax.random.permutation(jax.random.fold_in(seeds[5], 3), LAYERS * MB * TOKENS // TOK_DEV)
    expert_ids = jax.vmap(lambda own, number: deal_out(jax.random.fold_in(seeds[5], 2), own, number, TOK_DEV, EXPERTS, TOP, CAP, 0))(expert_ids_keys, expert_ids_turns).reshape((LAYERS, MB, TOKENS, TOP))
    route_weight = jnp.clip(jnp.exp(math.log(1.0) - 2.3025851 * jax.random.uniform(seeds[6], (LAYERS, MB, TOKENS, TOP), jnp.float32) ** block_scale(seeds[6], (LAYERS, MB, TOKENS, TOP), ((0, 8), (2, 32)), -0.2, 0.2)), 0.1, 1.0)
    return {"tokens": tokens, "norm_gain": norm_gain, "w_gate": w_gate, "w_up": w_up, "w_down": w_down, "expert_ids": expert_ids, "route_weight": route_weight}


epsilon = 1e-06

def expert_mlp(operands):
    inputs, gate_matrix, up_matrix, down_matrix = operands
    gate_proj = jnp.dot(inputs, gate_matrix, preferred_element_type=jnp.float32)
    upward = jnp.dot(inputs, up_matrix, preferred_element_type=jnp.float32)
    hidden = (jax.nn.silu(gate_proj) * upward).astype(jnp.bfloat16)
    return jnp.dot(hidden, down_matrix, preferred_element_type=jnp.float32).astype(jnp.bfloat16)

def layer_apply(residual, norm_scale, gate_all, up_all, down_all, route_ids, weights):
    values = residual.astype(jnp.float32)
    inverse_rms = lax.rsqrt(lax.optimization_barrier(jnp.mean(values * values, axis=-1, keepdims=True)) + epsilon)
    normed = (values * inverse_rms * norm_scale).astype(jnp.bfloat16)
    grouped = route_ids.reshape(N_EXPERT, TOK_DEV * TOP)
    onehot = (grouped[:, :, None] == jnp.arange(EXPERTS, dtype=jnp.int32)[None, None, :]).astype(jnp.int32)
    slot_index = lax.optimization_barrier(jnp.sum((jnp.cumsum(onehot, axis=1) - 1) * onehot, axis=-1))
    target = (jnp.arange(N_EXPERT, dtype=jnp.int32)[:, None] * CAP + slot_index).reshape(-1).astype(jnp.int32)
    chosen = route_ids.reshape(-1).astype(jnp.int32)
    owners = (jnp.arange(TOKENS * TOP, dtype=jnp.int32) // TOP).astype(jnp.int32)
    buffers = jnp.zeros((EXPERTS, N_EXPERT * CAP, D), jnp.bfloat16).at[chosen, target].set(normed[owners])
    results = lax.map(expert_mlp, (buffers, gate_all, up_all, down_all))
    picked = results[chosen, target].reshape(TOKENS, TOP, D).astype(jnp.float32)
    combined = values + lax.optimization_barrier(jnp.sum(weights[:, :, None] * picked, axis=1))
    return combined.astype(jnp.bfloat16)

def reference(tokens, norm_gain, w_gate, w_up, w_down, expert_ids, route_weight):
    states = [tokens[index] for index in range(MB)]
    layer_rows = []
    for layer in range(LAYERS):
        micro_rows = []
        for index in range(MB):
            states[index] = layer_apply(states[index], norm_gain[layer], w_gate[layer], w_up[layer], w_down[layer], expert_ids[layer, index], route_weight[layer, index])
            micro_rows.append(states[index])
        layer_rows.append(jnp.stack(micro_rows))
    return jnp.stack(layer_rows)
```

```python
import functools

import jax
import jax.numpy as jnp
from jax import lax
from jax.experimental import pallas as pl
from jax.experimental.pallas import tpu as pltpu
from jax.sharding import Mesh
from jax.sharding import PartitionSpec as P

EPS = 1e-06
D = 2048
HID = 704
HEAD = 640
TAIL = HID - HEAD
LANES = 2 * HID
ROWS = 3136
QUARTER = ROWS // 4
SLOTS = 32
LAYERS = 8


def pack_weights(gate, up, down):
    first = jnp.concatenate([gate[:, :HEAD], up[:, :HEAD], gate[:, HEAD:], up[:, HEAD:]], axis=1)
    second = down[:, :LANES]
    rest = down[:, LANES:]
    third = jnp.concatenate(
        [rest[:384], jnp.pad(rest[384:], ((0, 64), (0, 0))), jnp.zeros((384, 128), rest.dtype)], axis=1
    )
    return jnp.concatenate([first, second, third], axis=0)


def expert_kernel(where_ref, x_ref, *refs):
    sources, (out_ref, w, sems) = refs[:16], refs[16:]
    ahead, behind, core = where_ref[0], where_ref[1], where_ref[2]
    for quarter in range(4):
        half, way = quarter // 2, quarter % 2
        dist = ahead if way == 0 else behind
        for same in range(2):
            line = core == half if same == 0 else core != half
            for k in range(4):

                @pl.when(jnp.logical_and(line, dist == k))
                def _(src=sources[same * 8 + way * 4 + k], quarter=quarter):
                    pltpu.make_async_copy(src, w.at[pl.ds(quarter * QUARTER, QUARTER)], sems.at[quarter]).start()

    for quarter in range(4):
        pltpu.make_async_copy(sources[0], w.at[pl.ds(quarter * QUARTER, QUARTER)], sems.at[quarter]).wait()
    x = x_ref[...]
    h = jnp.dot(x, w[0:D, :], preferred_element_type=jnp.float32)
    gate, up = h[:, :HEAD], h[:, HEAD : 2 * HEAD]
    act_head = (gate / (1.0 + jnp.exp(-gate)) * up).astype(jnp.bfloat16)
    gate, up = h[:, 2 * HEAD : 2 * HEAD + TAIL], h[:, 2 * HEAD + TAIL :]
    act_tail = (gate / (1.0 + jnp.exp(-gate)) * up).astype(jnp.bfloat16)
    act = jnp.concatenate([act_head, act_tail], axis=1)
    out_ref[:, :LANES] = jnp.dot(act, w[D : D + HID, :], preferred_element_type=jnp.float32).astype(jnp.bfloat16)
    rest = jnp.dot(act[:, :384], w[D + HID : D + HID + 384, 0:640], preferred_element_type=jnp.float32)
    rest += jnp.dot(act[:, 384:], w[D + HID : D + HID + 320, 640:1280], preferred_element_type=jnp.float32)
    out_ref[:, LANES:] = rest.astype(jnp.bfloat16)


def expert_mlp(where, rows, sources):
    count = rows.shape[0]
    return pl.pallas_call(
        expert_kernel,
        out_shape=jax.ShapeDtypeStruct((count, D), jnp.bfloat16),
        in_specs=[pl.BlockSpec(memory_space=pltpu.SMEM), pl.BlockSpec(memory_space=pltpu.VMEM)]
        + [pl.BlockSpec(memory_space=pl.ANY)] * 16,
        out_specs=pl.BlockSpec(memory_space=pltpu.VMEM),
        scratch_shapes=[pltpu.VMEM((ROWS, LANES), jnp.bfloat16), pltpu.SemaphoreType.DMA((4,))],
        compiler_params=pltpu.CompilerParams(vmem_limit_bytes=40 * 2**20),
        cost_estimate=pl.CostEstimate(
            flops=2 * count * 3 * D * HID, bytes_accessed=ROWS * LANES * 2 + count * D * 4, transcendentals=count * HID
        ),
        name="expert_mlp",
    )(where, rows, *sources)


def per_device(tokens, norm_gain, w_gate, w_up, w_down, expert_ids, route_weight):
    section = lax.axis_index("section")
    xpos = lax.axis_index("x")
    plane, core = section // 2, section % 2
    micro, block = section // 4, section % 4
    tok = tokens.shape[1]
    quarter_tok = tok // 4

    ring_up = [(i, (i + 2) % 8) for i in range(8)]
    ring_down = [(i, (i - 2) % 8) for i in range(8)]
    partner = [(i, i ^ 1) for i in range(8)]

    def swap(v):
        return lax.ppermute(v, "section", partner)

    packed = pack_weights(w_gate[0, 0], w_up[0, 0], w_down[0, 0]).reshape(2, ROWS // 2, LANES)
    mine = lax.dynamic_index_in_dim(packed, core, 0, keepdims=False)
    other = lax.dynamic_index_in_dim(packed, 1 - core, 0, keepdims=False)
    received = swap(other)
    first = core == 0
    starts = (jnp.where(first, mine, received), jnp.where(first, received, mine))

    def spread(start):
        ahead, behind = [start[:QUARTER]], [start[QUARTER:]]
        for _ in range(3):
            ahead.append(lax.ppermute(ahead[-1], "section", ring_up))
            behind.append(lax.ppermute(behind[-1], "section", ring_down))
        return ahead + behind + [swap(v) for v in ahead] + [swap(v) for v in behind]

    chosen = lax.dynamic_index_in_dim(tokens, micro, 0, keepdims=False).reshape(4, quarter_tok, D)
    chosen = lax.all_to_all(chosen, "x", 0, 0, tiled=True)
    x = lax.dynamic_index_in_dim(chosen, block, 0, keepdims=False)
    routes = jnp.concatenate(
        [expert_ids[0].astype(jnp.float32), route_weight[0]], axis=-1
    ).transpose(0, 2, 1)
    routes = jnp.repeat(routes, 4, axis=0)
    routes = lax.all_to_all(routes, "section", 0, 0, tiled=True)
    routes = lax.all_gather(routes, "x", axis=0)
    routes = lax.dynamic_index_in_dim(routes, block, 0, keepdims=False)
    gains = lax.all_gather(norm_gain[0], "section", axis=0)
    ids = routes[:, :6].astype(jnp.int32)
    weights = routes[:, 6:]
    experts = jnp.arange(8, dtype=jnp.int32) * 4 + xpos
    hit = ids[:, None, :, :] == experts[None, :, None, None]
    named = hit.any(axis=2)
    weight = jnp.sum(jnp.where(hit, weights[:, None], 0.0), axis=2)
    earlier = jnp.triu(jnp.ones((tok, tok), jnp.bfloat16), 1)
    rank = jnp.dot(named.astype(jnp.bfloat16), earlier, preferred_element_type=jnp.float32).astype(jnp.int32)
    pick = jnp.logical_and(
        named[:, :, None], rank[:, :, None] == jnp.arange(SLOTS, dtype=jnp.int32)[None, None, :, None]
    )
    select = pick.astype(jnp.bfloat16).reshape(LAYERS, 8 * SLOTS, tok)
    spread_weight = jnp.where(pick, weight[:, :, None], 0.0).reshape(LAYERS, 8 * SLOTS, tok)
    high = spread_weight.astype(jnp.bfloat16)
    low = (spread_weight - high.astype(jnp.float32)).astype(jnp.bfloat16)
    gather_back = jnp.concatenate([high, low], axis=1)

    sources = [None, None]
    sources[0] = spread(starts[0])
    kept = []
    for layer in range(LAYERS):
        values = x.astype(jnp.float32)
        inverse = lax.rsqrt(jnp.mean(values * values, axis=-1, keepdims=True) + EPS)
        normed = (values * inverse * gains[layer]).astype(jnp.bfloat16)
        whole = lax.all_gather(normed, "x", axis=0, tiled=True)
        sent = jnp.dot(select[layer], whole, preferred_element_type=jnp.float32).astype(jnp.bfloat16)
        got = lax.all_to_all(sent.reshape(8, SLOTS, D), "z", 0, 0, tiled=True).reshape(8 * SLOTS, D)
        if layer == 0:
            sources[1] = spread(starts[1])
        home = layer // 2
        where = jnp.stack([(plane - home) % 4, (home - plane) % 4, core]).astype(jnp.int32)
        out = expert_mlp(where, got, sources[layer % 2])
        back = lax.all_to_all(out.reshape(8, SLOTS, D), "z", 0, 0, tiled=True).reshape(8 * SLOTS, D)
        both = jnp.concatenate([back, back], axis=0)
        part = lax.dot_general(
            gather_back[layer], both, (((0,), (0,)), ((), ())), preferred_element_type=jnp.float32
        ).astype(jnp.bfloat16)
        part = lax.all_to_all(part.reshape(4, quarter_tok, D), "x", 0, 0, tiled=True)
        x = (x.astype(jnp.float32) + jnp.sum(part.astype(jnp.float32), axis=0)).astype(jnp.bfloat16)
        kept.append(x)

    stream = lax.all_to_all(jnp.stack(kept), "section", 0, 0, tiled=True)
    stream = stream.reshape(2, 4, quarter_tok, D).transpose(1, 0, 2, 3)
    stream = lax.all_to_all(stream, "x", 0, 0, tiled=True)
    return stream.transpose(1, 0, 2, 3).reshape(1, 2, tok, D)


def solution(mesh):
    fine = Mesh(mesh.devices.reshape(8, 8, 4), ("section", "z", "x"))
    both = ("z", "x")
    return jax.shard_map(
        per_device,
        mesh=fine,
        in_specs=(
            P(None, both, None),
            P("section", None),
            P("section", both, None, None),
            P("section", both, None, None),
            P("section", both, None, None),
            P("section", None, both, None),
            P("section", None, both, None),
        ),
        out_specs=P("section", None, both, None),
        check_vma=False,
    )
```

```python
import jax
import jax.numpy as jnp
from jax import lax
from jax.experimental import pallas as pl
from jax.experimental.pallas import tpu as pltpu
from jax.sharding import Mesh
from jax.sharding import PartitionSpec as P

EPS = 1e-06
D = 2048
HID = 704
UP = 768
WIDE = 1536
TALL = 768
LAYERS = 8
CHUNKS = D // 128
ROWS = 200
PADDED = 208
DENSE = 400


VMEM = pl.BlockSpec(memory_space=pltpu.VMEM)


def pack_kernel(start_ref, gate_ref, up_ref, down_ref, out_ref):
    out_ref[0, 0:512, 0:HID] = gate_ref[...]
    out_ref[0, 0:512, HID:UP] = jnp.zeros((512, UP - HID), jnp.bfloat16)
    out_ref[0, 0:512, UP : UP + HID] = up_ref[...]
    out_ref[0, 0:512, UP + HID : WIDE] = jnp.zeros((512, WIDE - UP - HID), jnp.bfloat16)
    out_ref[0, 512:768, 0:512] = down_ref[0:256, :]
    out_ref[0, 512:768, 512:1024] = down_ref[256:512, :]
    out_ref[0, 512:704, 1024:1536] = down_ref[512:704, :]
    out_ref[0, 704:768, 1024:1536] = jnp.zeros((64, 512), jnp.bfloat16)


def pack_half(half, gate, up, down):
    return pl.pallas_call(
        pack_kernel,
        out_shape=jax.ShapeDtypeStruct((2, TALL, WIDE), jnp.bfloat16),
        grid_spec=pltpu.PrefetchScalarGridSpec(
            num_scalar_prefetch=1,
            grid=(2,),
            in_specs=[
                pl.BlockSpec((512, HID), lambda j, s: (s[0] + j, 0)),
                pl.BlockSpec((512, HID), lambda j, s: (s[0] + j, 0)),
                pl.BlockSpec((HID, 512), lambda j, s: (0, s[0] + j)),
            ],
            out_specs=pl.BlockSpec((1, TALL, WIDE), lambda j, s: (j, 0, 0)),
        ),
        compiler_params=pltpu.CompilerParams(vmem_limit_bytes=24 * 2**20),
        cost_estimate=pl.CostEstimate(flops=2 * 10**9, bytes_accessed=4 * TALL * WIDE * 2, transcendentals=0),
        name="pack_half",
    )((2 * half).reshape(1).astype(jnp.int32), gate, up, down)


def store_dense(rows_ref, out_ref, turn):
    for z in range(8):
        for j in range(16):
            out_ref[z, 16 * j : 16 * j + 16, :] = rows_ref[
                16 * z : 16 * z + 16, 128 * j : 128 * j + 128
            ].astype(jnp.bfloat16)
        for j in range(8):
            top = rows_ref[128 + 8 * z : 136 + 8 * z, 128 * j : 128 * j + 128]
            low = rows_ref[128 + 8 * z : 136 + 8 * z, 1024 + 128 * j : 1152 + 128 * j]
            out_ref[z, 256 + 16 * j : 272 + 16 * j, :] = jnp.concatenate([top, low], axis=0).astype(jnp.bfloat16)
    for j in range(CHUNKS):
        turn[8 * j : 8 * j + 8, :] = rows_ref[192:200, 128 * j : 128 * j + 128]
    for z in range(8):
        out_ref[z, 384:400, :] = turn[pl.ds(z, 16, stride=8), :].astype(jnp.bfloat16)


def load_dense(in_ref, rows_ref, turn):
    for z in range(8):
        for j in range(16):
            rows_ref[16 * z : 16 * z + 16, 128 * j : 128 * j + 128] = in_ref[z, 16 * j : 16 * j + 16, :]
    for z in range(0, 8, 2):
        for j in range(8):
            one = in_ref[z, 256 + 16 * j : 272 + 16 * j, :].astype(jnp.float32)
            two = in_ref[z + 1, 256 + 16 * j : 272 + 16 * j, :].astype(jnp.float32)
            rows = slice(128 + 8 * z, 144 + 8 * z)
            rows_ref[rows, 128 * j : 128 * j + 128] = jnp.concatenate([one[:8], two[:8]], axis=0).astype(jnp.bfloat16)
            rows_ref[rows, 1024 + 128 * j : 1152 + 128 * j] = jnp.concatenate([one[8:], two[8:]], axis=0).astype(
                jnp.bfloat16
            )
    for z in range(8):
        turn[pl.ds(z, 16, stride=8), :] = in_ref[z, 384:400, :].astype(jnp.float32)
    for j in range(CHUNKS):
        last = turn[8 * j : 8 * j + 8, :]
        rows_ref[192:208, 128 * j : 128 * j + 128] = jnp.concatenate([last, jnp.zeros_like(last)], axis=0).astype(
            jnp.bfloat16
        )


def dispatch_kernel(x_ref, gain_ref, select_ref, out_ref, rows, turn):
    values = x_ref[...].astype(jnp.float32)
    inverse = lax.rsqrt(jnp.mean(values * values, axis=-1, keepdims=True) + EPS)
    normed = (values * inverse * gain_ref[...]).astype(jnp.bfloat16)
    rows[...] = jnp.dot(select_ref[...], normed, preferred_element_type=jnp.float32)
    store_dense(rows, out_ref, turn)


def dispatch(x, gain, select):
    return pl.pallas_call(
        dispatch_kernel,
        out_shape=jax.ShapeDtypeStruct((8, DENSE, 128), jnp.bfloat16),
        in_specs=[VMEM] * 3,
        out_specs=VMEM,
        scratch_shapes=[pltpu.VMEM((ROWS, D), jnp.float32), pltpu.VMEM((128, 128), jnp.float32)],
        compiler_params=pltpu.CompilerParams(vmem_limit_bytes=16 * 2**20),
        cost_estimate=pl.CostEstimate(flops=10**9, bytes_accessed=2 * 10**6, transcendentals=128),
        name="dispatch",
    )(x, gain, select)


def expert_kernel(where_ref, in_ref, *refs):
    sources, (out_ref, w, x, rows, turn, sems) = refs[:16], refs[16:]
    dist, core = where_ref[0], where_ref[1]
    for quarter in range(4):
        half, part = quarter // 2, quarter % 2
        for same in range(2):
            line = core == half if same == 0 else core != half
            for k in range(4):

                @pl.when(jnp.logical_and(line, dist == k))
                def _(src=sources[same * 8 + part * 4 + k], quarter=quarter):
                    pltpu.make_async_copy(src, w.at[quarter], sems.at[quarter]).start()

    load_dense(in_ref, x, turn)
    gate = up = None
    for quarter in range(4):
        pltpu.make_async_copy(sources[0], w.at[quarter], sems.at[quarter]).wait()
        cut = x[:, 512 * quarter : 512 * quarter + 512]
        one = jnp.dot(cut, w[quarter, 0:512, 0:HID], preferred_element_type=jnp.float32)
        two = jnp.dot(cut, w[quarter, 0:512, UP : UP + HID], preferred_element_type=jnp.float32)
        gate, up = (one, two) if quarter == 0 else (gate + one, up + two)
    act = (gate / (1.0 + jnp.exp(-gate)) * up).astype(jnp.bfloat16)
    for quarter in range(4):
        out = jnp.dot(act[:, 0:256], w[quarter, 512:768, 0:512], preferred_element_type=jnp.float32)
        out += jnp.dot(act[:, 256:512], w[quarter, 512:768, 512:1024], preferred_element_type=jnp.float32)
        out += jnp.dot(act[:, 512:704], w[quarter, 512:704, 1024:1536], preferred_element_type=jnp.float32)
        rows[:, 512 * quarter : 512 * quarter + 512] = out
    store_dense(rows, out_ref, turn)


def expert_mlp(where, got, sources):
    return pl.pallas_call(
        expert_kernel,
        out_shape=jax.ShapeDtypeStruct((8, DENSE, 128), jnp.bfloat16),
        in_specs=[pl.BlockSpec(memory_space=pltpu.SMEM), VMEM] + [pl.BlockSpec(memory_space=pl.ANY)] * 16,
        out_specs=VMEM,
        scratch_shapes=[
            pltpu.VMEM((4, TALL, WIDE), jnp.bfloat16),
            pltpu.VMEM((PADDED, D), jnp.bfloat16),
            pltpu.VMEM((PADDED, D), jnp.float32),
            pltpu.VMEM((128, 128), jnp.float32),
            pltpu.SemaphoreType.DMA((4,)),
        ],
        compiler_params=pltpu.CompilerParams(vmem_limit_bytes=32 * 2**20),
        cost_estimate=pl.CostEstimate(
            flops=2 * PADDED * 3 * D * HID, bytes_accessed=4 * TALL * WIDE * 2, transcendentals=PADDED * HID
        ),
        name="expert_mlp",
    )(where, got, *sources)


def combine_kernel(in_ref, weight_ref, out_ref, x, turn):
    load_dense(in_ref, x, turn)
    back = x[0:ROWS, :]
    out = jnp.dot(weight_ref[0], back, preferred_element_type=jnp.float32)
    out += jnp.dot(weight_ref[1], back, preferred_element_type=jnp.float32)
    out_ref[...] = out.astype(jnp.bfloat16)


def combine(back, weight):
    return pl.pallas_call(
        combine_kernel,
        out_shape=jax.ShapeDtypeStruct((128, D), jnp.bfloat16),
        in_specs=[VMEM] * 2,
        out_specs=VMEM,
        scratch_shapes=[pltpu.VMEM((PADDED, D), jnp.bfloat16), pltpu.VMEM((128, 128), jnp.float32)],
        compiler_params=pltpu.CompilerParams(vmem_limit_bytes=16 * 2**20),
        cost_estimate=pl.CostEstimate(flops=10**9, bytes_accessed=2 * 10**6, transcendentals=0),
        name="combine",
    )(back, weight)


def per_slot(values):
    layers, _, tok = values.shape
    parts = [
        jnp.broadcast_to(values[:, :, None], (layers, 8, count, tok)).reshape(layers, 8 * count, tok)
        for count in (16, 8, 1)
    ]
    return jnp.concatenate(parts, axis=1)


def per_device(tokens, norm_gain, w_gate, w_up, w_down, expert_ids, route_weight):
    section = lax.axis_index("section")
    xpos = lax.axis_index("x")
    plane, core = section // 2, section % 2
    micro, block = section // 4, section % 4
    tok = tokens.shape[1]
    quarter_tok = tok // 4

    ring_up = [(i, (i + 2) % 8) for i in range(8)]
    ring_down = [(i, (i - 2) % 8) for i in range(8)]
    partner = [(i, i ^ 1) for i in range(8)]

    def swap(v):
        return lax.ppermute(v, "section", partner)

    def ahead(v):
        return lax.ppermute(v, "section", ring_up)

    def behind(v):
        return lax.ppermute(v, "section", ring_down)

    routes = jnp.concatenate([expert_ids[0].astype(jnp.float32), route_weight[0]], axis=-1).transpose(0, 2, 1)
    gain_rows = jnp.broadcast_to(norm_gain.reshape(1, D // 128, 128), (2, D // 128, 128))
    routes = jnp.concatenate([routes, gain_rows], axis=1)
    routes = jnp.repeat(routes, 4, axis=0)
    routes = lax.all_to_all(routes, "section", 0, 0, tiled=True)

    halves = (w_gate[0, 0], w_up[0, 0], w_down[0, 0])
    other = pack_half(1 - core, *halves)
    other, routes = lax.optimization_barrier((other, routes))
    received = swap(other)
    mine = pack_half(core, *halves)
    gains = routes[:, 12:].reshape(LAYERS, 1, D)
    routes = routes[:, :12]

    even = core == 0
    own = (
        (jnp.where(even, mine[0], received[0]), jnp.where(even, mine[1], received[1])),
        (jnp.where(even, received[0], mine[0]), jnp.where(even, received[1], mine[1])),
    )
    plane_even = plane % 2 == 0

    def first_hop(pair):
        return ahead(pair[0]), behind(pair[1])

    def second_hop(pair, hop, source):
        return ahead(jnp.where(source, pair[1], hop[0])), behind(jnp.where(source, pair[0], hop[1]))

    def after(values, done):
        return lax.optimization_barrier((values, done))

    def swapped(pair):
        return tuple(swap(v) for v in pair)

    hop1, hop2 = [None, None], {}
    hop1[0] = first_hop(own[0])
    hop2[0, 0] = second_hop(own[0], hop1[0], plane_even)
    odd_own, hop2[0, 0] = after(own[1], hop2[0, 0])
    hop1[1] = first_hop(odd_own)
    hop2[1, 0] = second_hop(odd_own, hop1[1], plane_even)
    (own0, hop1_0), hop2[1, 0] = after((own[0], hop1[0]), hop2[1, 0])
    hop2[0, 1] = second_hop(own0, hop1_0, jnp.logical_not(plane_even))
    (own1, hop1_1), hop2[0, 1] = after((odd_own, hop1[1]), hop2[0, 1])
    hop2[1, 1] = second_hop(own1, hop1_1, jnp.logical_not(plane_even))
    own = (own[0], odd_own)
    own_other = [swapped(own[0]), swapped(own[1])]
    hop1_other = [swapped(hop1[0]), swapped(hop1[1])]
    hop2_other = {key: swapped(hop2[key]) for key in hop2}

    def sources(layer):
        parity, late = layer % 2, (layer // 2) % 2
        order = []
        for mine, one, two in (
            (own[parity], hop1[parity], hop2[parity, late]),
            (own_other[parity], hop1_other[parity], hop2_other[parity, late]),
        ):
            order += [mine[0], one[0], two[0], two[1], mine[1], two[0], two[1], one[1]]
        return order

    chosen = lax.dynamic_index_in_dim(tokens, micro, 0, keepdims=False).reshape(4, quarter_tok, D)
    chosen = lax.all_to_all(chosen, "x", 0, 0, tiled=True)
    x = lax.dynamic_index_in_dim(chosen, block, 0, keepdims=False)
    routes = lax.all_gather(routes, "x", axis=0)
    routes = lax.dynamic_index_in_dim(routes, block, 0, keepdims=False)
    ids = routes[:, :6].astype(jnp.int32)
    weights = routes[:, 6:]
    experts = jnp.arange(8, dtype=jnp.int32) * 4 + xpos
    hit = ids[:, None, :, :] == experts[None, :, None, None]
    named = hit.any(axis=2)
    weight = jnp.sum(jnp.where(hit, weights[:, None], 0.0), axis=2)
    earlier = jnp.triu(jnp.ones((tok, tok), jnp.bfloat16), 1)
    rank = jnp.dot(named.astype(jnp.bfloat16), earlier, preferred_element_type=jnp.float32)
    rank = jnp.where(named, rank, -1.0)
    slot = jnp.concatenate(
        [jnp.tile(jnp.arange(16), 8), jnp.tile(jnp.arange(16, 24), 8), jnp.full((8,), 24)]
    ).astype(jnp.float32)
    pick = per_slot(rank) == slot[None, :, None]
    select = pick.astype(jnp.bfloat16)
    spread_weight = jnp.where(pick, per_slot(weight), 0.0).transpose(0, 2, 1)
    high = spread_weight.astype(jnp.bfloat16)
    low = (spread_weight - high.astype(jnp.float32)).astype(jnp.bfloat16)
    gather_back = jnp.stack([high, low], axis=1)

    def along_x(quarter):
        copies = jnp.broadcast_to(quarter[None], (4, quarter_tok, D))
        return lax.all_to_all(copies, "x", 0, 0, tiled=True).reshape(tok, D)

    everywhere = ("section", "z", "x")
    results = []

    def send_home(whole, layer):
        for m in range(2):
            route = [
                ((4 * m + xx) * 32 + z * 4 + xx, layer * 32 + z * 4 + xx) for z in range(8) for xx in range(4)
            ]
            results.append(lax.ppermute(whole, everywhere, route))

    for layer in range(LAYERS):
        whole = along_x(x)
        if layer > 0:
            send_home(whole, layer - 1)
        sent = dispatch(whole, gains[layer], select[layer])
        got = lax.all_to_all(sent, "z", 0, 0, tiled=True)
        where = jnp.stack([(plane - layer // 2) % 4, core]).astype(jnp.int32)
        out = expert_mlp(where, got, sources(layer))
        back = lax.all_to_all(out, "z", 0, 0, tiled=True)
        part = combine(back, gather_back[layer])
        part = lax.all_to_all(part.reshape(4, quarter_tok, D), "x", 0, 0, tiled=True)
        x = (x.astype(jnp.float32) + jnp.sum(part.astype(jnp.float32), axis=0)).astype(jnp.bfloat16)
    send_home(along_x(x), LAYERS - 1)
    stream = jnp.stack([sum(results[2::2], results[0]), sum(results[3::2], results[1])])
    return stream[None]


def solution(mesh):
    fine = Mesh(mesh.devices.reshape(8, 8, 4), ("section", "z", "x"))
    both = ("z", "x")
    return jax.shard_map(
        per_device,
        mesh=fine,
        in_specs=(
            P(None, both, None),
            P("section", None),
            P("section", both, None, None),
            P("section", both, None, None),
            P("section", both, None, None),
            P("section", None, both, None),
            P("section", None, both, None),
        ),
        out_specs=P("section", None, both, None),
        check_vma=False,
    )
```
